32 devices in a mesh: gx: 4 (over y, core), gy: 8 (over z, x).
Axes of the slice: x: 2, y: 2, z: 4, core: 2. Of those that a mesh axis runs over, the one named last changes fastest.
Arguments:
- wavefield: float32 [8, 16, 3, 125, 256], P('gx', 'gy'), may hold values from -0.6 to 0.6
- moduli: float32 [8, 16, 2, 256], P('gx', 'gy'), may hold values from 0.5 to 4
- residuals: float32 [32, 32, 128], P(('gx', 'gy')), may hold values from -6 to 6
- coords: float32 [32, 32, 3, 128], P(('gx', 'gy')), may hold values from -1 to 1
- angles: float32 [32, 32, 2, 128], P(('gx', 'gy')), may hold values from -3.140625 to 3.140625
- element_ids: int32 [32, 32, 128], P(('gx', 'gy')), may hold values from 0 to 1023
- counts: int32 [32, 32], P(('gx', 'gy')), may hold values from 0 to 128, as said below
Outputs:
- force: float32 [8, 16, 3, 125, 256], P('gx', 'gy')
The draws below stay inside these ranges and needn't reach their ends.
Inputs may be any that keep to these rules, and one draw needn't show every extreme that they name: `counts`: each sending device has at least one tile with exactly 128 live slots; in every draw one owner receives 128 live slots from every sender. The lightest owners receive on average about a sixth of 128 a sender, the others lie between.
All inputs are finite; a program needn't handle non-finite values.
Results may differ from the reference program's by a relative error of at most 0.0003.
Values sent between devices are 32-bit elements; how exact they have to be, the bound alone decides.
A program may use at most 64 MiB of HBM per device.

```python
import math
import jax
import jax.numpy as jnp
import numpy as np
from jax import lax

CX = 2
CY = 2
EZ = 256
CAP = 128
OWNERS = 32
NXE = 8
NYE = 16
N_GX = 4
N_GY = 8


def draw_counts(key, part):
    base_key = jax.random.fold_in(key, 11)
    key_heavy, key_base, key_full = jax.random.split(base_key, 3)
    heavy = jax.random.randint(key_heavy, (OWNERS,), 1, 5)
    base = jax.random.randint(key_base, (OWNERS, OWNERS), 0, CAP // 3 + 1)
    filled = jnp.minimum(base * heavy[None, :], CAP)
    full_owner = jax.random.randint(key_full, (), 0, OWNERS)
    column = jnp.arange(OWNERS, dtype=jnp.int32)[None, :]
    return jnp.where(column == full_owner, CAP, filled).astype(jnp.int32)


def set_ends(values, stream_key, least, high):
    spot = [jax.random.randint(jax.random.fold_in(stream_key, axis), (), 0, length) for axis, length in enumerate(values.shape)]
    longest = values.shape.index(max(values.shape))
    neighbour = spot[:longest] + [(spot[longest] + 1) % values.shape[longest]] + spot[longest + 1:]
    return values.at[tuple(spot)].set(least).at[tuple(neighbour)].set(high)


def steps_of(own_key, shape, cuts, least, largest):
    factor_of, own = 1.0, jax.random.fold_in(own_key, 6)
    for axis_at, blocks in cuts:
        heights = jnp.exp(jax.random.uniform(jax.random.fold_in(own, axis_at), (blocks,), jnp.float32, least / len(cuts), largest / len(cuts)))
        factor_of = factor_of * jnp.repeat(heights, shape[axis_at] // blocks).reshape([-1 if axis == axis_at else 1 for axis in range(len(shape))])
    return factor_of


def normal_values(own_key, dims, deviation, most, pieces=(), kind=jnp.bfloat16):
    level = steps_of(own_key, dims, pieces, -0.22, 0.18) if pieces else 1.0
    drawn = jax.random.normal(own_key, dims, jnp.float32) * deviation * level
    return jnp.minimum(jnp.maximum(drawn, -most), most).astype(kind)


def setup_inputs(seed: int = 0) -> dict:
    key_of = jax.random.split(jax.random.key(seed), 8)
    wavefield = normal_values(key_of[0], (NXE, NYE, 3, 125, EZ), 0.1, 0.6, ((0, 4), (1, 8)), jnp.float32)
    moduli = jnp.clip(jnp.exp(math.log(4.0) - 2.0794415 * jax.random.uniform(key_of[1], (NXE, NYE, 2, EZ), jnp.float32) ** steps_of(key_of[1], (NXE, NYE, 2, EZ), ((0, 4), (1, 8)), -0.2, 0.2)), 0.5, 4.0)
    residuals = normal_values(key_of[2], (OWNERS, OWNERS, CAP), 1.0, 6.0, ((0, 32),), jnp.float32)
    coords = jnp.clip(jax.random.uniform(key_of[3], (OWNERS, OWNERS, 3, CAP), jnp.float32, -1.0, 1.0) * steps_of(key_of[3], (OWNERS, OWNERS, 3, CAP), ((0, 32),), -0.4, 0.0), -1.0, 1.0)
    angles = jnp.clip(jax.random.uniform(key_of[4], (OWNERS, OWNERS, 2, CAP), jnp.float32, -3.140625, 3.140625), -3.140625, 3.140625)
    element_ids = set_ends(jax.random.randint(key_of[5], (OWNERS, OWNERS, CAP), 0, CX * CY * EZ), jax.random.fold_in(key_of[5], 1), 0, (CX * CY * EZ) - 1).astype(jnp.int32)
    counts = draw_counts(jax.random.fold_in(key_of[7], 71), 0)
    return dict(wavefield=wavefield, moduli=moduli, residuals=residuals, coords=coords, angles=angles, element_ids=element_ids, counts=counts)


def gll_points():
    return np.array([-1.0, -math.sqrt(3.0 / 7.0), 0.0, math.sqrt(3.0 / 7.0), 1.0])

def gll_weights():
    return np.array([0.1, 49.0 / 90.0, 32.0 / 45.0, 49.0 / 90.0, 0.1])

def derivative_table():
    points = gll_points()
    table = np.zeros((5, 5))
    for row in range(5):
        for col in range(5):
            if row == col:
                table[row, col] = sum((1.0 / (points[col] - points[other]) for other in range(5) if other != col))
            else:
                value = 1.0 / (points[col] - points[row])
                for other in range(5):
                    if other != col and other != row:
                        value = value * (points[row] - points[other]) / (points[col] - points[other])
                table[row, col] = value
    return table

def basis(where):
    points = gll_points()
    values = []
    slopes = []
    for node in range(5):
        value = jnp.ones_like(where)
        slope = jnp.zeros_like(where)
        for other in range(5):
            if other != node:
                scale = 1.0 / (points[node] - points[other])
                factor = (where - points[other]) * scale
                slope = slope * factor + value * scale
                value = value * factor
        values.append(value)
        slopes.append(slope)
    return (jnp.stack(values), jnp.stack(slopes))

def inject(total, resid, coord, angle, ids, live_count):
    slots = resid.shape[-1]
    live = jnp.arange(slots, dtype=jnp.int32)[None, :] < live_count[:, None]
    value = jnp.where(live, resid, 0.0).reshape(-1)
    first = coord[:, 0, :].reshape(-1)
    second = coord[:, 1, :].reshape(-1)
    third = coord[:, 2, :].reshape(-1)
    azimuth = angle[:, 0, :].reshape(-1)
    dip = angle[:, 1, :].reshape(-1)
    tang_x = jnp.cos(azimuth) * jnp.cos(dip)
    tang_y = jnp.sin(azimuth) * jnp.cos(dip)
    tang_z = jnp.sin(dip)
    val_x, der_x = basis(first)
    val_y, der_y = basis(second)
    val_z, der_z = basis(third)
    shape = tang_x * der_x[:, None, None, :] * val_y[None, :, None, :] * val_z[None, None, :, :] + tang_y * val_x[:, None, None, :] * der_y[None, :, None, :] * val_z[None, None, :, :] + tang_z * val_x[:, None, None, :] * val_y[None, :, None, :] * der_z[None, None, :, :]
    direction = jnp.stack([tang_x, tang_y, tang_z]) * value[None, :]
    contrib = (direction[:, None, None, None, :] * shape[None]).reshape(375, -1)
    return total.at[:, ids.reshape(-1)].add(contrib)

def along(field, table, dim):
    if dim == 0:
        return jnp.einsum('pa,...aqsz->...pqsz', table, field, precision=lax.Precision.HIGHEST)
    if dim == 1:
        return jnp.einsum('qb,...pbsz->...pqsz', table, field, precision=lax.Precision.HIGHEST)
    return jnp.einsum('sc,...pqcz->...pqsz', table, field, precision=lax.Precision.HIGHEST)

def back(field, table, dim):
    if dim == 0:
        return jnp.einsum('pa,...pqsz->...aqsz', table, field, precision=lax.Precision.HIGHEST)
    if dim == 1:
        return jnp.einsum('qb,...pqsz->...pbsz', table, field, precision=lax.Precision.HIGHEST)
    return jnp.einsum('sc,...pqsz->...pqcz', table, field, precision=lax.Precision.HIGHEST)

def stiffness(field, moduli):
    table = jnp.asarray(derivative_table(), jnp.float32)
    weight = jnp.asarray(gll_weights(), jnp.float32)
    wgrid = (weight[:, None, None] * weight[None, :, None] * weight[None, None, :])[:, :, :, None]
    grads = [along(field, table, dim) for dim in range(3)]
    lame = moduli[..., 0, :][..., None, None, None, :]
    shear = moduli[..., 1, :][..., None, None, None, :]
    diverge = grads[0][..., 0, :, :, :, :] + grads[1][..., 1, :, :, :, :] + grads[2][..., 2, :, :, :, :]
    result = jnp.zeros_like(field)
    for col in range(3):
        parts = []
        for row in range(3):
            stress = shear * (grads[col][..., row, :, :, :, :] + grads[row][..., col, :, :, :, :])
            if row == col:
                stress = stress + lame * diverge
            parts.append(stress * wgrid)
        result = result + back(jnp.stack(parts, axis=-5), table, col)
    return result

def assemble_dim(field, e_dim, n_dim, fetch):
    count = field.shape[e_dim]
    low = lax.slice_in_dim(field, 0, 1, axis=n_dim)
    high = lax.slice_in_dim(field, 4, 5, axis=n_dim)
    middle = lax.slice_in_dim(field, 1, 4, axis=n_dim)
    first = lax.slice_in_dim(low, 0, 1, axis=e_dim)
    last = lax.slice_in_dim(high, count - 1, count, axis=e_dim)
    below, above = fetch(first, last)
    low_next = jnp.concatenate([lax.slice_in_dim(low, 1, count, axis=e_dim), above], axis=e_dim)
    high_prev = jnp.concatenate([below, lax.slice_in_dim(high, 0, count - 1, axis=e_dim)], axis=e_dim)
    return jnp.concatenate([low + high_prev, middle, high + low_next], axis=n_dim)

def fetch_none(first, last):
    return (jnp.zeros_like(last), jnp.zeros_like(first))

def reference(wavefield, moduli, residuals, coords, angles, element_ids, counts):
    owners = N_GX * N_GY
    nxe = CX * N_GX
    nye = CY * N_GY
    index = jnp.arange(owners, dtype=jnp.int32)
    owner_x = (index // N_GY)[:, None]
    owner_y = (index % N_GY)[:, None]

    def per_source(total, items):
        resid, coord, angle, ids, live_count = items
        cell_x = ids // (CY * EZ)
        cell_y = ids // EZ % CY
        cell_z = ids % EZ
        global_ids = (((owner_x * CX + cell_x) * nye + owner_y * CY + cell_y) * EZ + cell_z).astype(jnp.int32)
        return (inject(total, resid, coord, angle, global_ids, live_count), None)
    start = jnp.zeros((375, nxe * nye * EZ), jnp.float32)
    total, unused = lax.scan(per_source, start, (residuals, coords, angles, element_ids, counts))
    injected = total.reshape(3, 5, 5, 5, nxe, nye, EZ).transpose(4, 5, 0, 1, 2, 3, 6)
    field = wavefield.reshape(nxe, nye, 3, 5, 5, 5, EZ)
    internal = lax.map(lambda pair: stiffness(pair[0], pair[1]), (field, moduli))
    force = injected - internal
    force = assemble_dim(force, 0, 3, fetch_none)
    force = assemble_dim(force, 1, 4, fetch_none)
    force = assemble_dim(force, 6, 5, fetch_none)
    return force.reshape(nxe, nye, 3, 125, EZ)
```

```python
import functools
import math

import jax
import jax.numpy as jnp
import numpy as np
from jax import lax
from jax.experimental import pallas as pl
from jax.experimental.pallas import tpu as pltpu
from jax.sharding import PartitionSpec as P

MESH = pl.DeviceIdType.MESH
F32, BF16 = jnp.float32, jnp.bfloat16
PAD = 128
GROUP = 8


def gll_points():
    return np.array([-1.0, -math.sqrt(3.0 / 7.0), 0.0, math.sqrt(3.0 / 7.0), 1.0])


def gll_weights():
    return np.array([0.1, 49.0 / 90.0, 32.0 / 45.0, 49.0 / 90.0, 0.1])


def derivative_table():
    points = gll_points()
    table = np.zeros((5, 5))
    for row in range(5):
        for col in range(5):
            if row == col:
                table[row, col] = sum(
                    (1.0 / (points[col] - points[other]) for other in range(5) if other != col)
                )
            else:
                value = 1.0 / (points[col] - points[row])
                for other in range(5):
                    if other != col and other != row:
                        value = (
                            value * (points[row] - points[other]) / (points[col] - points[other])
                        )
                table[row, col] = value
    return table


def split_table(table):
    high = table.astype(BF16)
    return high, (table - high.astype(np.float64)).astype(BF16)


def tables():
    dm, eye = derivative_table(), np.eye(5)
    w1 = gll_weights()
    weight = (w1[:, None, None] * w1[None, :, None] * w1[None, None, :]).reshape(-1)
    dirs = [
        np.kron(np.kron(dm, eye), eye),
        np.kron(np.kron(eye, dm), eye),
        np.kron(np.kron(eye, eye), dm),
    ]
    grad = np.zeros((3 * PAD, PAD))
    back = np.zeros((PAD, 3 * PAD))
    for j in range(3):
        grad[j * PAD : j * PAD + 125, :125] = dirs[j]
        back[:125, j * PAD : j * PAD + 125] = -dirs[j].T * weight[None, :]
    gh, gl = split_table(grad)
    bh, bl = split_table(back)
    g1 = np.concatenate([gh, gh], 1)
    bs = np.concatenate([bh, bl], 0)
    spread = np.zeros((4 * PAD, 192))
    for p in range(5):
        for q in range(5):
            for r in range(5):
                n = (p * 5 + q) * 5 + r
                for base, col in ((0, p * 8 + q), (1, 40 + p * 8 + q), (2, 80 + r), (3, 88 + r)):
                    spread[base * PAD + n, col] = 1.0
                    spread[base * PAD + n, 96 + col] = 1.0
    points = gll_points()
    consts = np.zeros((8, 8, 128), np.float32)
    for q in range(5):
        others = [k for k in range(5) if k != q]
        for j, k in enumerate(others):
            consts[j, q] = points[k]
            consts[4 + j, q] = 1.0 / (points[q] - points[k])
    return (
        jnp.asarray(g1),
        jnp.asarray(gl),
        jnp.asarray(bs),
        jnp.asarray(spread.astype(BF16)),
        jnp.asarray(consts),
    )


def split(x):
    high = x.astype(BF16)
    return high, (x - high.astype(F32)).astype(BF16)


def dot(a, b):
    return jnp.dot(a, b, preferred_element_type=F32)


def dot_t(a, b):
    return lax.dot_general(a, b, (((1,), (1,)), ((), ())), preferred_element_type=F32)


def scatter_kernel(nx, ny, resid, coord, angle, ids, count, recv, packed, got, send_sem, recv_sem):
    n = nx * ny
    gx, gy = lax.axis_index("gx"), lax.axis_index("gy")
    me = gx * ny + gy
    barrier = pltpu.get_barrier_semaphore()

    def greet(k, c):
        to = lax.rem(me + k, n)
        pl.semaphore_signal(
            barrier, inc=1, device_id=(to // ny, lax.rem(to, ny)), device_id_type=MESH
        )
        return c

    lax.fori_loop(1, n, greet, 0)
    slots = resid.shape[2]
    rows = lax.broadcasted_iota(jnp.int32, (n, n), 0)
    cols = lax.broadcasted_iota(jnp.int32, (n, n), 1)
    spread = jnp.where(rows == cols, count[...].astype(F32), 0.0)
    live_count = jnp.sum(spread, axis=1, keepdims=True)
    slot = lax.broadcasted_iota(jnp.int32, (n, slots), 1).astype(F32)
    az, dip = angle[0, :, 0, :], angle[0, :, 1, :]
    cd = jnp.cos(dip)
    packed[:, 0, :] = jnp.where(slot < live_count, resid[0], 0.0)
    for d in range(3):
        packed[:, 1 + d, :] = coord[0, :, d, :]
    packed[:, 4, :] = jnp.cos(az) * cd
    packed[:, 5, :] = jnp.sin(az) * cd
    packed[:, 6, :] = jnp.sin(dip)
    packed[:, 7, :] = ids[0].astype(F32)
    pl.semaphore_wait(barrier, n - 1)

    def copy(k, to, at):
        return pltpu.make_async_remote_copy(
            src_ref=packed.at[to],
            dst_ref=got.at[at],
            send_sem=send_sem.at[k],
            recv_sem=recv_sem.at[k],
            device_id=(to // ny, lax.rem(to, ny)),
            device_id_type=MESH,
        )

    def send(k, c):
        copy(k, lax.rem(me + k, n), me).start()
        return c

    lax.fori_loop(1, n, send, 0)
    recv[me] = packed[me]

    def finish(k, c):
        frm = lax.rem(me - k + n, n)
        copy(k, lax.rem(me + k, n), frm).wait_recv()
        recv[frm] = got[frm]
        return c

    lax.fori_loop(1, n, finish, 0)

    def drain(k, c):
        copy(k, lax.rem(me + k, n), me).wait_send()
        return c

    lax.fori_loop(1, n, drain, 0)


def basis(row, const):
    x = jnp.broadcast_to(row, const[0].shape)
    value = slope = None
    for j in range(4):
        scale = const[4 + j]
        factor = (x - const[j]) * scale
        if value is None:
            value, slope = factor, scale
        else:
            slope = slope * factor + value * scale
            value = value * factor
    return value, slope


def force_kernel(
    cx, cy, u_ref, mod_ref, recv, g1, g2, bs, spread, consts, out, xs, ys, cs, acc, lhs, hot, pad
):
    n, slots = recv.shape[0], recv.shape[2]
    cells, depth = cx * cy, u_ref.shape[3]
    width = 2 * slots
    acc[...] = jnp.zeros_like(acc)
    pad[...] = jnp.zeros_like(pad)

    def block(b, carry):
        for pair in range(GROUP // 2):
            at = b * GROUP + 2 * pair
            tile = jnp.concatenate([recv[at], recv[at + 1]], axis=1)
            const = [
                jnp.concatenate([consts[j], consts[j]], axis=1) for j in range(8)
            ]
            v = tile[0:1]
            t = [tile[4 + i : 5 + i] for i in range(3)]
            lx, dx = basis(tile[1:2], const)
            ly, dy = basis(tile[2:3], const)
            lz, dz = basis(tile[3:4], const)
            dx, dy, dz = dx * t[0], dy * t[1], dz * t[2]
            first = [dx[p : p + 1] * ly + lx[p : p + 1] * dy for p in range(5)]
            second = [lx[p : p + 1] * ly for p in range(5)]
            high, low = split(jnp.concatenate(first + second + [lz, dz], axis=0))
            wide = dot(spread[...], jnp.concatenate([high, low], axis=0))
            shape = wide[:PAD] * wide[2 * PAD : 3 * PAD] + wide[PAD : 2 * PAD] * wide[3 * PAD :]
            cols = pl.ds(pair * width, width)
            for i in range(3):
                high, low = split(shape * (v * t[i]))
                lhs[i * PAD : (i + 1) * PAD, cols] = high
                lhs[(3 + i) * PAD : (4 + i) * PAD, cols] = low
            ident = tile[7:8].astype(jnp.int32)
            number = lax.broadcasted_iota(jnp.int32, (cells * depth, width), 0)
            hot[:, cols] = jnp.where(number == ident, 1.0, 0.0).astype(BF16)
        for cell in range(cells):
            got = dot_t(lhs[...], hot[cell * depth : (cell + 1) * depth, :])
            acc[cell] += got[: 3 * PAD] + got[3 * PAD :]
        return carry

    lax.fori_loop(0, n // GROUP, block, 0)

    node = lax.broadcasted_iota(jnp.int32, (PAD, depth), 0)
    lane = lax.broadcasted_iota(jnp.int32, (PAD, depth), 1)
    along = lax.rem(node, 5)
    take_up = (along == 4) & (lane < depth - 1)
    take_down = (along == 0) & (lane > 0)

    def stiff(cell, carry):
        g = []
        for c in range(3):
            pad[0:125, :] = u_ref[cell, c]
            high, low = split(pad[...])
            r = dot(g1[...], jnp.concatenate([high, low], axis=0)) + dot(g2[...], high)
            g.append([r[j * PAD : (j + 1) * PAD] for j in range(3)])
        lam, mu = mod_ref[cell, 0:1, :], mod_ref[cell, 1:2, :]
        press = lam * (g[0][0] + g[1][1] + g[2][2])
        for i in range(3):
            parts = []
            for j in range(3):
                s = mu * (g[i][j] + g[j][i])
                parts.append(s + press if i == j else s)
            high, low = split(jnp.concatenate(parts, axis=0))
            r = dot(bs[...], high)
            r = r[:PAD] + r[PAD:] + dot(bs[:PAD], low)
            f = acc[cell, i * PAD : (i + 1) * PAD, :] + r
            up = pltpu.roll(pltpu.roll(f, depth - 1, 1), 4, 0)
            down = pltpu.roll(pltpu.roll(f, 1, 1), PAD - 4, 0)
            f = f + jnp.where(take_up, up, 0.0) + jnp.where(take_down, down, 0.0)
            acc[cell, i * PAD : (i + 1) * PAD, :] = f
        return carry

    lax.fori_loop(0, cells, stiff, 0)

    def join(a, ra, b, rb, size):
        total = acc[a, ra : ra + size, :] + acc[b, rb : rb + size, :]
        acc[a, ra : ra + size, :] = total
        acc[b, rb : rb + size, :] = total

    for c in range(3):
        o = c * PAD
        for y in range(cy):
            for x in range(cx - 1):
                join(x * cy + y, o + 100, (x + 1) * cy + y, o, 25)
        for x in range(cx):
            for y in range(cy - 1):
                for p in range(5):
                    join(x * cy + y, o + p * 25 + 20, x * cy + y + 1, o + p * 25, 5)
        for y in range(cy):
            xs[0, y, c] = acc[y, o : o + 25, :]
            xs[1, y, c] = acc[(cx - 1) * cy + y, o + 100 : o + 125, :]
        for x in range(cx):
            for p in range(5):
                k = o + p * 25
                ys[0, x, c, p * 5 : p * 5 + 5, :] = acc[x * cy, k : k + 5, :]
                ys[1, x, c, p * 5 : p * 5 + 5, :] = acc[x * cy + cy - 1, k + 20 : k + 25, :]
        for x in range(2):
            for y in range(2):
                cell = x * (cx - 1) * cy + y * (cy - 1)
                k = o + x * 100 + y * 20
                cs[x, y, c] = acc[cell, k : k + 5, :]
        for cell in range(cells):
            out[cell, c] = acc[cell, o : o + 125, :]


def halo_kernel(nx, ny, xs, ys, cs, rx, ry, rc, send_sem, recv_sem):
    gx, gy = lax.axis_index("gx"), lax.axis_index("gy")
    moves = []
    for side in (0, 1):
        moves.append((2 * side - 1, 0, xs.at[side], rx.at[1 - side], rx.at[side]))
    for side in (0, 1):
        moves.append((0, 2 * side - 1, ys.at[side], ry.at[1 - side], ry.at[side]))
    for x in (0, 1):
        for y in (0, 1):
            moves.append((2 * x - 1, 2 * y - 1, cs.at[x, y], rc.at[1 - x, 1 - y], rc.at[x, y]))
    opposite = [1, 0, 3, 2, 7, 6, 5, 4]
    barrier = pltpu.get_barrier_semaphore()

    def there(dx, dy):
        ok = None
        for pos, step, count in ((gx, dx, nx), (gy, dy, ny)):
            if step:
                c = pos > 0 if step < 0 else pos < count - 1
                ok = c if ok is None else ok & c
        return ok

    waits = jnp.int32(0)
    for dx, dy, src, dst, mine in moves:
        @pl.when(there(dx, dy))
        def _():
            pl.semaphore_signal(barrier, inc=1, device_id=(gx + dx, gy + dy), device_id_type=MESH)

        waits = waits + there(dx, dy).astype(jnp.int32)
    pl.semaphore_wait(barrier, waits)

    def copy(m, at, landing):
        dx, dy, src, dst, mine = moves[m]
        return pltpu.make_async_remote_copy(
            src_ref=src,
            dst_ref=landing,
            send_sem=send_sem.at[m],
            recv_sem=recv_sem.at[at],
            device_id=(gx + dx, gy + dy),
            device_id_type=MESH,
        )

    for m, (dx, dy, src, dst, mine) in enumerate(moves):
        @pl.when(there(dx, dy))
        def _():
            copy(m, m, dst).start()

        @pl.when(jnp.logical_not(there(dx, dy)))
        def _():
            mine[...] = jnp.zeros_like(mine)

    for m, (dx, dy, src, dst, mine) in enumerate(moves):
        @pl.when(there(dx, dy))
        def _():
            copy(m, opposite[m], mine).wait_recv()
            copy(m, m, dst).wait_send()


def join_kernel(cx, cy, field, rx, ry, rc, out):
    out[...] = field[...]
    for c in range(3):
        for y in range(cy):
            out[y, c, 0:25, :] += rx[0, y, c]
            out[(cx - 1) * cy + y, c, 100:125, :] += rx[1, y, c]
        for x in range(cx):
            for p in range(5):
                k = p * 25
                out[x * cy, c, k : k + 5, :] += ry[0, x, c, p * 5 : p * 5 + 5, :]
                out[x * cy + cy - 1, c, k + 20 : k + 25, :] += ry[1, x, c, p * 5 : p * 5 + 5, :]
        for x in range(2):
            for y in range(2):
                cell = x * (cx - 1) * cy + y * (cy - 1)
                k = x * 100 + y * 20
                out[cell, c, k : k + 5, :] += rc[x, y, c]


def vmem(count):
    return [pl.BlockSpec(memory_space=pltpu.VMEM)] * count


def body(nx, ny, wavefield, moduli, residuals, coords, angles, element_ids, counts):
    cx, cy, depth = wavefield.shape[0], wavefield.shape[1], wavefield.shape[4]
    n, slots = nx * ny, residuals.shape[2]
    cells = cx * cy
    shape = jax.ShapeDtypeStruct
    recv = pl.pallas_call(
        functools.partial(scatter_kernel, nx, ny),
        out_shape=shape((n, 8, slots), F32),
        in_specs=vmem(5),
        out_specs=vmem(1)[0],
        scratch_shapes=[
            pltpu.VMEM((n, 8, slots), F32),
            pltpu.VMEM((n, 8, slots), F32),
            pltpu.SemaphoreType.DMA((n,)),
            pltpu.SemaphoreType.DMA((n,)),
        ],
        compiler_params=pltpu.CompilerParams(collective_id=0, has_side_effects=True),
    )(residuals, coords, angles, element_ids, counts)
    strips = (
        shape((2, cy, 3, 25, depth), F32),
        shape((2, cx, 3, 25, depth), F32),
        shape((2, 2, 3, 5, depth), F32),
    )
    field, xs, ys, cs = pl.pallas_call(
        functools.partial(force_kernel, cx, cy),
        out_shape=(shape((cells, 3, 125, depth), F32),) + strips,
        in_specs=vmem(8),
        out_specs=tuple(vmem(4)),
        scratch_shapes=[
            pltpu.VMEM((cells, 3 * PAD, depth), F32),
            pltpu.VMEM((6 * PAD, GROUP * slots), BF16),
            pltpu.VMEM((cells * depth, GROUP * slots), BF16),
            pltpu.VMEM((PAD, depth), F32),
        ],
    )(
        wavefield.reshape(cells, 3, 125, depth),
        moduli.reshape(cells, 2, depth),
        recv,
        *tables(),
    )
    rx, ry, rc = pl.pallas_call(
        functools.partial(halo_kernel, nx, ny),
        out_shape=strips,
        in_specs=vmem(3),
        out_specs=tuple(vmem(3)),
        scratch_shapes=[pltpu.SemaphoreType.DMA((8,)), pltpu.SemaphoreType.DMA((8,))],
        compiler_params=pltpu.CompilerParams(collective_id=1, has_side_effects=True),
    )(xs, ys, cs)
    force = pl.pallas_call(
        functools.partial(join_kernel, cx, cy),
        out_shape=shape((cells, 3, 125, depth), F32),
        in_specs=vmem(4),
        out_specs=vmem(1)[0],
    )(field, rx, ry, rc)
    return force.reshape(cx, cy, 3, 125, depth)


def solution(mesh):
    in_specs = (
        P("gx", "gy", None, None, None),
        P("gx", "gy", None, None),
        P(("gx", "gy"), None, None),
        P(("gx", "gy"), None, None, None),
        P(("gx", "gy"), None, None, None),
        P(("gx", "gy"), None, None),
        P(("gx", "gy"), None),
    )
    out_specs = P("gx", "gy", None, None, None)
    return jax.shard_map(
        functools.partial(body, mesh.shape["gx"], mesh.shape["gy"]),
        mesh=mesh,
        in_specs=in_specs,
        out_specs=out_specs,
        check_vma=False,
    )
```

```python
import functools
import math

import jax
import jax.numpy as jnp
import numpy as np
from jax import lax
from jax.experimental import pallas as pl
from jax.experimental.pallas import tpu as pltpu
from jax.sharding import PartitionSpec as P

MESH = pl.DeviceIdType.MESH
F32, BF16 = jnp.float32, jnp.bfloat16
PAD = 128
SPAN = 32


def gll_points():
    return np.array([-1.0, -math.sqrt(3.0 / 7.0), 0.0, math.sqrt(3.0 / 7.0), 1.0])


def gll_weights():
    return np.array([0.1, 49.0 / 90.0, 32.0 / 45.0, 49.0 / 90.0, 0.1])


def derivative_table():
    points = gll_points()
    table = np.zeros((5, 5))
    for row in range(5):
        for col in range(5):
            if row == col:
                table[row, col] = sum(
                    (1.0 / (points[col] - points[other]) for other in range(5) if other != col)
                )
            else:
                value = 1.0 / (points[col] - points[row])
                for other in range(5):
                    if other != col and other != row:
                        value = (
                            value * (points[row] - points[other]) / (points[col] - points[other])
                        )
                table[row, col] = value
    return table


def split_table(table):
    high = table.astype(BF16)
    return high, (table - high.astype(np.float64)).astype(BF16)


def tables():
    dm, eye = derivative_table(), np.eye(5)
    w1 = gll_weights()
    weight = (w1[:, None, None] * w1[None, :, None] * w1[None, None, :]).reshape(-1)
    dirs = [
        np.kron(np.kron(dm, eye), eye),
        np.kron(np.kron(eye, dm), eye),
        np.kron(np.kron(eye, eye), dm),
    ]
    grad = np.zeros((3 * PAD, PAD))
    back = np.zeros((PAD, 3 * PAD))
    for j in range(3):
        grad[j * PAD : j * PAD + 125, :125] = dirs[j]
        back[:125, j * PAD : j * PAD + 125] = -dirs[j].T * weight[None, :]
    gh, gl = split_table(grad)
    bh, bl = split_table(back)
    g1 = np.concatenate([gh, gh], 1)
    bs = np.concatenate([bh, bl], 0)
    spread = np.zeros((4 * PAD, 192))
    for p in range(5):
        for q in range(5):
            for r in range(5):
                n = (p * 5 + q) * 5 + r
                for base, col in ((0, p * 8 + q), (1, 40 + p * 8 + q), (2, 80 + r), (3, 88 + r)):
                    spread[base * PAD + n, col] = 1.0
                    spread[base * PAD + n, 96 + col] = 1.0
    points = gll_points()
    consts = np.zeros((8, 8, 128), np.float32)
    for q in range(5):
        others = [k for k in range(5) if k != q]
        for j, k in enumerate(others):
            consts[j, q] = points[k]
            consts[4 + j, q] = 1.0 / (points[q] - points[k])
    return (
        jnp.asarray(g1),
        jnp.asarray(gl),
        jnp.asarray(bs),
        jnp.asarray(spread.astype(BF16)),
        jnp.asarray(consts),
    )


def split(x):
    high = x.astype(BF16)
    return high, (x - high.astype(F32)).astype(BF16)


def dot(a, b):
    return jnp.dot(a, b, preferred_element_type=F32)


def dot_t(a, b):
    return lax.dot_general(a, b, (((1,), (1,)), ((), ())), preferred_element_type=F32)


def basis(row, const):
    x = jnp.broadcast_to(row, const[0].shape)
    value = slope = None
    for j in range(4):
        scale = const[4 + j]
        factor = (x - const[j]) * scale
        if value is None:
            value, slope = factor, scale
        else:
            slope = slope * factor + value * scale
            value = value * factor
    return value, slope


def step_kernel(
    nx, ny, cx, cy, resid, coord, angle, ids, count, u_ref, mod_ref, g1, g2, bs, spread, consts,
    out, packed, got, acc, lhs, hot, pad, xs, ys, cs, rx, ry, rc,
    send_sem, recv_sem, halo_send, halo_recv,
):
    n = nx * ny
    gx, gy = lax.axis_index("gx"), lax.axis_index("gy")
    me = gx * ny + gy
    cells, depth, slots = cx * cy, acc.shape[2], resid.shape[2]
    halves = depth // 128
    rows_node = halves * cy
    span = min(n, SPAN)
    width = 2 * slots
    barrier = pltpu.get_barrier_semaphore()

    def greet(k, c):
        to = lax.rem(me + k, n)
        pl.semaphore_signal(
            barrier, inc=1, device_id=(to // ny, lax.rem(to, ny)), device_id_type=MESH
        )
        return c

    lax.fori_loop(1, n, greet, 0)
    rows = lax.broadcasted_iota(jnp.int32, (n, n), 0)
    cols = lax.broadcasted_iota(jnp.int32, (n, n), 1)
    diagonal = jnp.where(rows == cols, count[...].astype(F32), 0.0)
    live_count = jnp.sum(diagonal, axis=1, keepdims=True)
    slot = lax.broadcasted_iota(jnp.int32, (n, slots), 1).astype(F32)
    az, dip = angle[0, :, 0, :], angle[0, :, 1, :]
    cd = jnp.cos(dip)
    packed[:, 0, :] = jnp.where(slot < live_count, resid[0], 0.0)
    for d in range(3):
        packed[:, 1 + d, :] = coord[0, d]
    packed[:, 4, :] = jnp.cos(az) * cd
    packed[:, 5, :] = jnp.sin(az) * cd
    packed[:, 6, :] = jnp.sin(dip)
    packed[:, 7, :] = ids[0].astype(F32)
    pl.semaphore_wait(barrier, n - 1)

    def tile_copy(k, to, at):
        return pltpu.make_async_remote_copy(
            src_ref=packed.at[to],
            dst_ref=got.at[at],
            send_sem=send_sem.at[k],
            recv_sem=recv_sem.at[k],
            device_id=(to // ny, lax.rem(to, ny)),
            device_id_type=MESH,
        )

    def send(k, c):
        tile_copy(k, lax.rem(me + k, n), me).start()
        return c

    lax.fori_loop(1, n, send, 0)
    got[me] = packed[me]

    pad[...] = jnp.zeros_like(pad)

    def stiff(cell, carry):
        g = []
        for c in range(3):
            start = ((cell // cy) * 3 + c) * 125 * rows_node + lax.rem(cell, cy)
            for h in range(halves):
                pad[0:125, h * 128 : (h + 1) * 128] = u_ref[
                    pl.ds(start + h * cy, 125, stride=rows_node), :
                ]
            high, low = split(pad[...])
            r = dot(g1[...], jnp.concatenate([high, low], axis=0)) + dot(g2[...], high)
            g.append([r[j * PAD : (j + 1) * PAD] for j in range(3)])
        lam, mu = mod_ref[cell, 0:1, :], mod_ref[cell, 1:2, :]
        press = lam * (g[0][0] + g[1][1] + g[2][2])
        for i in range(3):
            parts = []
            for j in range(3):
                s = mu * (g[i][j] + g[j][i])
                parts.append(s + press if i == j else s)
            high, low = split(jnp.concatenate(parts, axis=0))
            r = dot(bs[...], high)
            acc[cell, i * PAD : (i + 1) * PAD, :] = r[:PAD] + r[PAD:] + dot(bs[:PAD], low)
        return carry

    lax.fori_loop(0, cells, stiff, 0)

    def arrive(k, c):
        tile_copy(k, lax.rem(me + k, n), lax.rem(me - k + n, n)).wait_recv()
        return c

    lax.fori_loop(1, n, arrive, 0)

    def prepare(first_tile):
        def pair(k, carry):
            at = first_tile + 2 * k
            tile = jnp.concatenate([got[at], got[at + 1]], axis=1)
            const = [jnp.concatenate([consts[j], consts[j]], axis=1) for j in range(8)]
            v = tile[0:1]
            t = [tile[4 + i : 5 + i] for i in range(3)]
            lx, dx = basis(tile[1:2], const)
            ly, dy = basis(tile[2:3], const)
            lz, dz = basis(tile[3:4], const)
            dx, dy, dz = dx * t[0], dy * t[1], dz * t[2]
            first = [dx[p : p + 1] * ly + lx[p : p + 1] * dy for p in range(5)]
            second = [lx[p : p + 1] * ly for p in range(5)]
            high, low = split(jnp.concatenate(first + second + [lz, dz], axis=0))
            wide = dot(spread[...], jnp.concatenate([high, low], axis=0))
            shape = wide[:PAD] * wide[2 * PAD : 3 * PAD] + wide[PAD : 2 * PAD] * wide[3 * PAD :]
            cols = pl.ds(pl.multiple_of(k * width, width), width)
            for i in range(3):
                high, low = split(shape * (v * t[i]))
                lhs[i, :PAD, cols] = high
                lhs[i, PAD:, cols] = low
            ident = tile[7:8].astype(jnp.int32)
            number = lax.broadcasted_iota(jnp.int32, (cells * depth, width), 0)
            hot[:, cols] = jnp.where(number == ident, 1.0, 0.0).astype(BF16)
            return carry

        lax.fori_loop(0, span // 2, pair, 0)

    def gather(i, cell):
        r = dot_t(lhs[i], hot[cell * depth : (cell + 1) * depth, :])
        return acc[cell, i * PAD : (i + 1) * PAD, :] + r[:PAD] + r[PAD:]

    if n > span:
        def early(b, carry):
            prepare(b * span)
            for i in range(3):
                for cell in range(cells):
                    acc[cell, i * PAD : (i + 1) * PAD, :] = gather(i, cell)
            return carry

        lax.fori_loop(0, n // span - 1, early, 0)
    prepare(n - span)

    node = lax.broadcasted_iota(jnp.int32, (PAD, depth), 0)
    lane = lax.broadcasted_iota(jnp.int32, (PAD, depth), 1)
    along = lax.rem(node, 5)
    take_up = (along == 4) & (lane < depth - 1)
    take_down = (along == 0) & (lane > 0)

    def join(a, ra, b, rb, size):
        total = acc[a, ra : ra + size, :] + acc[b, rb : rb + size, :]
        acc[a, ra : ra + size, :] = total
        acc[b, rb : rb + size, :] = total

    moves = []
    for side in (0, 1):
        moves.append((2 * side - 1, 0, xs, rx, (side,), (1 - side,)))
    for side in (0, 1):
        moves.append((0, 2 * side - 1, ys, ry, (side,), (1 - side,)))
    for x in (0, 1):
        for y in (0, 1):
            moves.append((2 * x - 1, 2 * y - 1, cs, rc, (x, y), (1 - x, 1 - y)))
    opposite = [1, 0, 3, 2, 7, 6, 5, 4]

    def there(m):
        ok = None
        for pos, step, total in ((gx, moves[m][0], nx), (gy, moves[m][1], ny)):
            if step:
                c = pos > 0 if step < 0 else pos < total - 1
                ok = c if ok is None else ok & c
        return ok

    def strip_copy(c, m, sem, place):
        dx, dy, src, dst, mine, theirs = moves[m]
        return pltpu.make_async_remote_copy(
            src_ref=src.at[(c,) + mine],
            dst_ref=dst.at[(c,) + place],
            send_sem=halo_send.at[c * 8 + m],
            recv_sem=halo_recv.at[c * 8 + sem],
            device_id=(gx + dx, gy + dy),
            device_id_type=MESH,
        )

    for m in range(8):
        @pl.when(jnp.logical_not(there(m)))
        def _():
            dst, mine = moves[m][3], moves[m][4]
            for c in range(3):
                hole = dst.at[(c,) + mine]
                hole[...] = jnp.zeros(hole.shape, F32)

    for c in range(3):
        o = c * PAD
        for cell in range(cells):
            f = gather(c, cell)
            up = pltpu.roll(pltpu.roll(f, depth - 1, 1), 4, 0)
            down = pltpu.roll(pltpu.roll(f, 1, 1), PAD - 4, 0)
            acc[cell, o : o + PAD, :] = (
                f + jnp.where(take_up, up, 0.0) + jnp.where(take_down, down, 0.0)
            )
        for y in range(cy):
            for x in range(cx - 1):
                join(x * cy + y, o + 100, (x + 1) * cy + y, o, 25)
        for x in range(cx):
            for y in range(cy - 1):
                for p in range(5):
                    join(x * cy + y, o + p * 25 + 20, x * cy + y + 1, o + p * 25, 5)
        for y in range(cy):
            xs[c, 0, y] = acc[y, o : o + 25, :]
            xs[c, 1, y] = acc[(cx - 1) * cy + y, o + 100 : o + 125, :]
        for x in range(cx):
            for p in range(5):
                k = o + p * 25
                ys[c, 0, x, p * 5 : p * 5 + 5, :] = acc[x * cy, k : k + 5, :]
                ys[c, 1, x, p * 5 : p * 5 + 5, :] = acc[x * cy + cy - 1, k + 20 : k + 25, :]
        for x in range(2):
            for y in range(2):
                cell = x * (cx - 1) * cy + y * (cy - 1)
                k = o + x * 100 + y * 20
                cs[c, x, y] = acc[cell, k : k + 5, :]
        for m in range(8):
            @pl.when(there(m))
            def _():
                strip_copy(c, m, m, moves[m][5]).start()

    def drain(k, c):
        tile_copy(k, lax.rem(me + k, n), me).wait_send()
        return c

    lax.fori_loop(1, n, drain, 0)

    for c in range(3):
        o = c * PAD
        for m in range(8):
            @pl.when(there(m))
            def _():
                strip_copy(c, m, opposite[m], moves[m][4]).wait_recv()
                strip_copy(c, m, m, moves[m][5]).wait_send()

        for y in range(cy):
            acc[y, o : o + 25, :] += rx[c, 0, y]
            acc[(cx - 1) * cy + y, o + 100 : o + 125, :] += rx[c, 1, y]
        for x in range(cx):
            for p in range(5):
                k = o + p * 25
                acc[x * cy, k : k + 5, :] += ry[c, 0, x, p * 5 : p * 5 + 5, :]
                acc[x * cy + cy - 1, k + 20 : k + 25, :] += ry[c, 1, x, p * 5 : p * 5 + 5, :]
        for x in range(2):
            for y in range(2):
                cell = x * (cx - 1) * cy + y * (cy - 1)
                k = o + x * 100 + y * 20
                acc[cell, k : k + 5, :] += rc[c, x, y]
        for cell in range(cells):
            start = ((cell // cy) * 3 + c) * 125 * rows_node + cell % cy
            for h in range(halves):
                out[pl.ds(start + h * cy, 125, stride=rows_node), :] = acc[
                    cell, o : o + 125, h * 128 : (h + 1) * 128
                ]


def vmem(count):
    return [pl.BlockSpec(memory_space=pltpu.VMEM)] * count


def body(nx, ny, wavefield, moduli, residuals, coords, angles, element_ids, counts):
    cx, cy, depth = wavefield.shape[0], wavefield.shape[1], wavefield.shape[4]
    n, slots = nx * ny, residuals.shape[2]
    cells, halves = cx * cy, depth // 128
    span = min(n, SPAN)
    rows = wavefield.transpose(0, 2, 3, 1, 4).reshape(cx, 3, 125, cy, halves, 128)
    rows = rows.transpose(0, 1, 2, 4, 3, 5).reshape(-1, 128)
    scratch = [
        pltpu.VMEM((n, 8, slots), F32),
        pltpu.VMEM((n, 8, slots), F32),
        pltpu.VMEM((cells, 3 * PAD, depth), F32),
        pltpu.VMEM((3, 2 * PAD, span * slots), BF16),
        pltpu.VMEM((cells * depth, span * slots), BF16),
        pltpu.VMEM((PAD, depth), F32),
    ]
    for _ in range(2):
        scratch += [
            pltpu.VMEM((3, 2, cy, 25, depth), F32),
            pltpu.VMEM((3, 2, cx, 25, depth), F32),
            pltpu.VMEM((3, 2, 2, 5, depth), F32),
        ]
    scratch += [
        pltpu.SemaphoreType.DMA((n,)),
        pltpu.SemaphoreType.DMA((n,)),
        pltpu.SemaphoreType.DMA((24,)),
        pltpu.SemaphoreType.DMA((24,)),
    ]
    force = pl.pallas_call(
        functools.partial(step_kernel, nx, ny, cx, cy),
        out_shape=jax.ShapeDtypeStruct(rows.shape, F32),
        in_specs=vmem(12),
        out_specs=vmem(1)[0],
        scratch_shapes=scratch,
        compiler_params=pltpu.CompilerParams(collective_id=0, has_side_effects=True),
    )(
        residuals,
        coords.transpose(0, 2, 1, 3),
        angles,
        element_ids,
        counts,
        rows,
        moduli.reshape(cells, 2, depth),
        *tables(),
    )
    force = force.reshape(cx, 3, 125, halves, cy, 128).transpose(0, 1, 2, 4, 3, 5)
    return force.reshape(cx, 3, 125, cy, depth).transpose(0, 3, 1, 2, 4)


def solution(mesh):
    in_specs = (
        P("gx", "gy", None, None, None),
        P("gx", "gy", None, None),
        P(("gx", "gy"), None, None),
        P(("gx", "gy"), None, None, None),
        P(("gx", "gy"), None, None, None),
        P(("gx", "gy"), None, None),
        P(("gx", "gy"), None),
    )
    out_specs = P("gx", "gy", None, None, None)
    return jax.shard_map(
        functools.partial(body, mesh.shape["gx"], mesh.shape["gy"]),
        mesh=mesh,
        in_specs=in_specs,
        out_specs=out_specs,
        check_vma=False,
    )
```

```python
import functools
import math

import jax
import jax.numpy as jnp
import numpy as np
from jax import lax
from jax.experimental import pallas as pl
from jax.experimental.pallas import tpu as pltpu
from jax.sharding import PartitionSpec as P

MESH = pl.DeviceIdType.MESH
F32, BF16 = jnp.float32, jnp.bfloat16
PAD = 128
SPAN = 32


def gll_points():
    return np.array([-1.0, -math.sqrt(3.0 / 7.0), 0.0, math.sqrt(3.0 / 7.0), 1.0])


def gll_weights():
    return np.array([0.1, 49.0 / 90.0, 32.0 / 45.0, 49.0 / 90.0, 0.1])


def derivative_table():
    points = gll_points()
    table = np.zeros((5, 5))
    for row in range(5):
        for col in range(5):
            if row == col:
                table[row, col] = sum(
                    (1.0 / (points[col] - points[other]) for other in range(5) if other != col)
                )
            else:
                value = 1.0 / (points[col] - points[row])
                for other in range(5):
                    if other != col and other != row:
                        value = (
                            value * (points[row] - points[other]) / (points[col] - points[other])
                        )
                table[row, col] = value
    return table


def split_table(table):
    high = table.astype(BF16)
    return high, (table - high.astype(np.float64)).astype(BF16)


def tables():
    dm, eye = derivative_table(), np.eye(5)
    w1 = gll_weights()
    weight = (w1[:, None, None] * w1[None, :, None] * w1[None, None, :]).reshape(-1)
    dirs = [
        np.kron(np.kron(dm, eye), eye),
        np.kron(np.kron(eye, dm), eye),
        np.kron(np.kron(eye, eye), dm),
    ]
    grad = np.zeros((3 * PAD, PAD))
    back = np.zeros((PAD, 3 * PAD))
    for j in range(3):
        grad[j * PAD : j * PAD + 125, :125] = dirs[j]
        back[:125, j * PAD : j * PAD + 125] = -dirs[j].T * weight[None, :]
    gh, gl = split_table(grad)
    bh, bl = split_table(back)
    g1 = np.concatenate([gh, gh], 1)
    bs = np.concatenate([bh, bl], 0)
    spread = np.zeros((4 * PAD, 192))
    for p in range(5):
        for q in range(5):
            for r in range(5):
                n = (p * 5 + q) * 5 + r
                for base, col in ((0, p * 8 + q), (1, 40 + p * 8 + q), (2, 80 + r), (3, 88 + r)):
                    spread[base * PAD + n, col] = 1.0
                    spread[base * PAD + n, 96 + col] = 1.0
    points = gll_points()
    consts = np.zeros((8, 8, 128), np.float32)
    for q in range(5):
        others = [k for k in range(5) if k != q]
        for j, k in enumerate(others):
            consts[j, q] = points[k]
            consts[4 + j, q] = 1.0 / (points[q] - points[k])
    return (
        jnp.asarray(g1),
        jnp.asarray(gl),
        jnp.asarray(bs),
        jnp.asarray(spread.astype(BF16)),
        jnp.asarray(consts),
    )


def split(x):
    high = x.astype(BF16)
    return high, (x - high.astype(F32)).astype(BF16)


def dot(a, b):
    return jnp.dot(a, b, preferred_element_type=F32)


def dot_t(a, b):
    return lax.dot_general(a, b, (((1,), (1,)), ((), ())), preferred_element_type=F32)


def basis(row, const):
    x = jnp.broadcast_to(row, const[0].shape)
    value = slope = None
    for j in range(4):
        scale = const[4 + j]
        factor = (x - const[j]) * scale
        if value is None:
            value, slope = factor, scale
        else:
            slope = slope * factor + value * scale
            value = value * factor
    return value, slope


def step_kernel(
    nx, ny, cx, cy, resid, coord, angle, ids, count, u_ref, mod_ref, g1, g2, bs, spread, consts,
    out, packed, got, acc, lhs, hot, pad, xs, ys, cs, rx, ry, rc,
    send_sem, recv_sem, halo_send, halo_recv,
):
    n = nx * ny
    gx, gy = lax.axis_index("gx"), lax.axis_index("gy")
    me = gx * ny + gy
    cells, depth, slots = cx * cy, acc.shape[2], resid.shape[2]
    halves = depth // 128
    rows_node = halves * cy
    span = min(n, SPAN)
    width = 2 * slots
    barrier = pltpu.get_barrier_semaphore()

    def greet(k, c):
        to = lax.rem(me + k, n)
        pl.semaphore_signal(
            barrier, inc=1, device_id=(to // ny, lax.rem(to, ny)), device_id_type=MESH
        )
        return c

    lax.fori_loop(1, n, greet, 0)
    rows = lax.broadcasted_iota(jnp.int32, (n, n), 0)
    cols = lax.broadcasted_iota(jnp.int32, (n, n), 1)
    diagonal = jnp.where(rows == cols, count[...].astype(F32), 0.0)
    live_count = jnp.sum(diagonal, axis=1, keepdims=True)
    slot = lax.broadcasted_iota(jnp.int32, (n, slots), 1).astype(F32)
    az, dip = angle[0, :, 0, :], angle[0, :, 1, :]
    cd = jnp.cos(dip)
    packed[:, 0, :] = jnp.where(slot < live_count, resid[0], 0.0)
    for d in range(3):
        packed[:, 1 + d, :] = coord[0, d]
    packed[:, 4, :] = jnp.cos(az) * cd
    packed[:, 5, :] = jnp.sin(az) * cd
    packed[:, 6, :] = jnp.sin(dip)
    packed[:, 7, :] = ids[0].astype(F32)
    pad[...] = jnp.zeros_like(pad)

    def stiff(cell, carry):
        g = []
        for c in range(3):
            start = ((cell // cy) * 3 + c) * 125 * rows_node + lax.rem(cell, cy)
            for h in range(halves):
                pad[0:125, h * 128 : (h + 1) * 128] = u_ref[
                    pl.ds(start + h * cy, 125, stride=rows_node), :
                ]
            high, low = split(pad[...])
            r = dot(g1[...], jnp.concatenate([high, low], axis=0)) + dot(g2[...], high)
            g.append([r[j * PAD : (j + 1) * PAD] for j in range(3)])
        lam, mu = mod_ref[cell, 0:1, :], mod_ref[cell, 1:2, :]
        press = lam * (g[0][0] + g[1][1] + g[2][2])
        for i in range(3):
            parts = []
            for j in range(3):
                s = mu * (g[i][j] + g[j][i])
                parts.append(s + press if i == j else s)
            high, low = split(jnp.concatenate(parts, axis=0))
            r = dot(bs[...], high)
            acc[cell, i * PAD : (i + 1) * PAD, :] = r[:PAD] + r[PAD:] + dot(bs[:PAD], low)
        return carry

    lax.fori_loop(0, cells // 2, stiff, 0)
    pl.semaphore_wait(barrier, n - 1)

    def tile_copy(k, to, at):
        return pltpu.make_async_remote_copy(
            src_ref=packed.at[to],
            dst_ref=got.at[at],
            send_sem=send_sem.at[k],
            recv_sem=recv_sem.at[k],
            device_id=(to // ny, lax.rem(to, ny)),
            device_id_type=MESH,
        )

    def send(k, c):
        tile_copy(k, lax.rem(me + k, n), me).start()
        return c

    lax.fori_loop(1, n, send, 0)
    got[me] = packed[me]

    lax.fori_loop(cells // 2, cells, stiff, 0)

    def arrive(k, c):
        tile_copy(k, lax.rem(me + k, n), lax.rem(me - k + n, n)).wait_recv()
        return c

    lax.fori_loop(1, n, arrive, 0)

    def prepare(first_tile):
        def pair(k, carry):
            at = first_tile + 2 * k
            tile = jnp.concatenate([got[at], got[at + 1]], axis=1)
            const = [jnp.concatenate([consts[j], consts[j]], axis=1) for j in range(8)]
            v = tile[0:1]
            t = [tile[4 + i : 5 + i] for i in range(3)]
            lx, dx = basis(tile[1:2], const)
            ly, dy = basis(tile[2:3], const)
            lz, dz = basis(tile[3:4], const)
            dx, dy, dz = dx * t[0], dy * t[1], dz * t[2]
            first = [dx[p : p + 1] * ly + lx[p : p + 1] * dy for p in range(5)]
            second = [lx[p : p + 1] * ly for p in range(5)]
            high, low = split(jnp.concatenate(first + second + [lz, dz], axis=0))
            wide = dot(spread[...], jnp.concatenate([high, low], axis=0))
            shape = wide[:PAD] * wide[2 * PAD : 3 * PAD] + wide[PAD : 2 * PAD] * wide[3 * PAD :]
            cols = pl.ds(pl.multiple_of(k * width, width), width)
            for i in range(3):
                high, low = split(shape * (v * t[i]))
                lhs[i, :PAD, cols] = high
                lhs[i, PAD:, cols] = low
            ident = tile[7:8].astype(jnp.int32)
            number = lax.broadcasted_iota(jnp.int32, (cells * depth, width), 0)
            hot[:, cols] = jnp.where(number == ident, 1.0, 0.0).astype(BF16)
            return carry

        lax.fori_loop(0, span // 2, pair, 0)

    def gather(i, cell):
        r = dot_t(lhs[i], hot[cell * depth : (cell + 1) * depth, :])
        return acc[cell, i * PAD : (i + 1) * PAD, :] + r[:PAD] + r[PAD:]

    if n > span:
        def early(b, carry):
            prepare(b * span)
            for i in range(3):
                for cell in range(cells):
                    acc[cell, i * PAD : (i + 1) * PAD, :] = gather(i, cell)
            return carry

        lax.fori_loop(0, n // span - 1, early, 0)
    prepare(n - span)

    node = lax.broadcasted_iota(jnp.int32, (PAD, depth), 0)
    lane = lax.broadcasted_iota(jnp.int32, (PAD, depth), 1)
    along = lax.rem(node, 5)
    take_up = (along == 4) & (lane < depth - 1)
    take_down = (along == 0) & (lane > 0)

    def join(a, ra, b, rb, size):
        total = acc[a, ra : ra + size, :] + acc[b, rb : rb + size, :]
        acc[a, ra : ra + size, :] = total
        acc[b, rb : rb + size, :] = total

    moves = []
    for side in (0, 1):
        moves.append((2 * side - 1, 0, xs, rx, (side,), (1 - side,)))
    for side in (0, 1):
        moves.append((0, 2 * side - 1, ys, ry, (side,), (1 - side,)))
    for x in (0, 1):
        for y in (0, 1):
            moves.append((2 * x - 1, 2 * y - 1, cs, rc, (x, y), (1 - x, 1 - y)))
    opposite = [1, 0, 3, 2, 7, 6, 5, 4]

    def there(m):
        ok = None
        for pos, step, total in ((gx, moves[m][0], nx), (gy, moves[m][1], ny)):
            if step:
                c = pos > 0 if step < 0 else pos < total - 1
                ok = c if ok is None else ok & c
        return ok

    def strip_copy(c, m, sem, place):
        dx, dy, src, dst, mine, theirs = moves[m]
        return pltpu.make_async_remote_copy(
            src_ref=src.at[(c,) + mine],
            dst_ref=dst.at[(c,) + place],
            send_sem=halo_send.at[c * 8 + m],
            recv_sem=halo_recv.at[c * 8 + sem],
            device_id=(gx + dx, gy + dy),
            device_id_type=MESH,
        )

    for m in range(8):
        @pl.when(jnp.logical_not(there(m)))
        def _():
            dst, mine = moves[m][3], moves[m][4]
            for c in range(3):
                hole = dst.at[(c,) + mine]
                hole[...] = jnp.zeros(hole.shape, F32)

    for c in range(3):
        o = c * PAD
        for cell in range(cells):
            f = gather(c, cell)
            up = pltpu.roll(pltpu.roll(f, depth - 1, 1), 4, 0)
            down = pltpu.roll(pltpu.roll(f, 1, 1), PAD - 4, 0)
            acc[cell, o : o + PAD, :] = (
                f + jnp.where(take_up, up, 0.0) + jnp.where(take_down, down, 0.0)
            )
        for y in range(cy):
            for x in range(cx - 1):
                join(x * cy + y, o + 100, (x + 1) * cy + y, o, 25)
        for x in range(cx):
            for y in range(cy - 1):
                for p in range(5):
                    join(x * cy + y, o + p * 25 + 20, x * cy + y + 1, o + p * 25, 5)
        for y in range(cy):
            xs[c, 0, y] = acc[y, o : o + 25, :]
            xs[c, 1, y] = acc[(cx - 1) * cy + y, o + 100 : o + 125, :]
        for x in range(cx):
            for p in range(5):
                k = o + p * 25
                ys[c, 0, x, p * 5 : p * 5 + 5, :] = acc[x * cy, k : k + 5, :]
                ys[c, 1, x, p * 5 : p * 5 + 5, :] = acc[x * cy + cy - 1, k + 20 : k + 25, :]
        for x in range(2):
            for y in range(2):
                cell = x * (cx - 1) * cy + y * (cy - 1)
                k = o + x * 100 + y * 20
                cs[c, x, y] = acc[cell, k : k + 5, :]
        for m in range(8):
            @pl.when(there(m))
            def _():
                strip_copy(c, m, m, moves[m][5]).start()

    def drain(k, c):
        tile_copy(k, lax.rem(me + k, n), me).wait_send()
        return c

    lax.fori_loop(1, n, drain, 0)

    for c in range(3):
        o = c * PAD
        for m in range(8):
            @pl.when(there(m))
            def _():
                strip_copy(c, m, opposite[m], moves[m][4]).wait_recv()
                strip_copy(c, m, m, moves[m][5]).wait_send()

        for y in range(cy):
            acc[y, o : o + 25, :] += rx[c, 0, y]
            acc[(cx - 1) * cy + y, o + 100 : o + 125, :] += rx[c, 1, y]
        for x in range(cx):
            for p in range(5):
                k = o + p * 25
                acc[x * cy, k : k + 5, :] += ry[c, 0, x, p * 5 : p * 5 + 5, :]
                acc[x * cy + cy - 1, k + 20 : k + 25, :] += ry[c, 1, x, p * 5 : p * 5 + 5, :]
        for x in range(2):
            for y in range(2):
                cell = x * (cx - 1) * cy + y * (cy - 1)
                k = o + x * 100 + y * 20
                acc[cell, k : k + 5, :] += rc[c, x, y]
        for cell in range(cells):
            start = ((cell // cy) * 3 + c) * 125 * rows_node + cell % cy
            for h in range(halves):
                out[pl.ds(start + h * cy, 125, stride=rows_node), :] = acc[
                    cell, o : o + 125, h * 128 : (h + 1) * 128
                ]


def vmem(count):
    return [pl.BlockSpec(memory_space=pltpu.VMEM)] * count


def body(nx, ny, wavefield, moduli, residuals, coords, angles, element_ids, counts):
    cx, cy, depth = wavefield.shape[0], wavefield.shape[1], wavefield.shape[4]
    n, slots = nx * ny, residuals.shape[2]
    cells, halves = cx * cy, depth // 128
    span = min(n, SPAN)
    rows = wavefield.transpose(0, 2, 3, 1, 4).reshape(cx, 3, 125, cy, halves, 128)
    rows = rows.transpose(0, 1, 2, 4, 3, 5).reshape(-1, 128)
    scratch = [
        pltpu.VMEM((n, 8, slots), F32),
        pltpu.VMEM((n, 8, slots), F32),
        pltpu.VMEM((cells, 3 * PAD, depth), F32),
        pltpu.VMEM((3, 2 * PAD, span * slots), BF16),
        pltpu.VMEM((cells * depth, span * slots), BF16),
        pltpu.VMEM((PAD, depth), F32),
    ]
    for _ in range(2):
        scratch += [
            pltpu.VMEM((3, 2, cy, 25, depth), F32),
            pltpu.VMEM((3, 2, cx, 25, depth), F32),
            pltpu.VMEM((3, 2, 2, 5, depth), F32),
        ]
    scratch += [
        pltpu.SemaphoreType.DMA((n,)),
        pltpu.SemaphoreType.DMA((n,)),
        pltpu.SemaphoreType.DMA((24,)),
        pltpu.SemaphoreType.DMA((24,)),
    ]
    force = pl.pallas_call(
        functools.partial(step_kernel, nx, ny, cx, cy),
        out_shape=jax.ShapeDtypeStruct(rows.shape, F32),
        in_specs=vmem(12),
        out_specs=vmem(1)[0],
        scratch_shapes=scratch,
        compiler_params=pltpu.CompilerParams(collective_id=0, has_side_effects=True),
    )(
        residuals,
        coords.transpose(0, 2, 1, 3),
        angles,
        element_ids,
        counts,
        rows,
        moduli.reshape(cells, 2, depth),
        *tables(),
    )
    force = force.reshape(cx, 3, 125, halves, cy, 128).transpose(0, 1, 2, 4, 3, 5)
    return force.reshape(cx, 3, 125, cy, depth).transpose(0, 3, 1, 2, 4)


def solution(mesh):
    in_specs = (
        P("gx", "gy", None, None, None),
        P("gx", "gy", None, None),
        P(("gx", "gy"), None, None),
        P(("gx", "gy"), None, None, None),
        P(("gx", "gy"), None, None, None),
        P(("gx", "gy"), None, None),
        P(("gx", "gy"), None),
    )
    out_specs = P("gx", "gy", None, None, None)
    return jax.shard_map(
        functools.partial(body, mesh.shape["gx"], mesh.shape["gy"]),
        mesh=mesh,
        in_specs=in_specs,
        out_specs=out_specs,
        check_vma=False,
    )
```
